32 devices in a mesh: tm: 32 (over z, y, x, core), prod: 1.
Axes of the slice: x: 2, y: 2, z: 4, core: 2. Of those that a mesh axis runs over, the one named last changes fastest.
Arguments:
- sales_records: float32 [1024, 16, 16, 128], P('tm', 'prod'), may hold values from -6 to 6
- day_month: int32 [1024], replicated, may hold values from 0 to 31, as said below
- month_year: int32 [32], replicated, may hold values from 0 to 3, never falling along the last dimension, each value on 1 to 16 neighbouring positions
- product_category: int32 [16], replicated, may hold values from 0 to 31
- store_region: int32 [16], replicated, may hold values from 0 to 3
Outputs:
- month_detail: float32 [32, 32, 4, 128], P('tm', 'prod')
- month_category: float32 [32, 32, 128], P('tm', 'prod')
- month_region: float32 [32, 4, 128], P('tm')
- month_totals: float32 [32, 128], P('tm')
- year_detail: float32 [4, 32, 4, 128], replicated
- year_category: float32 [4, 32, 128], replicated
- year_region: float32 [4, 4, 128], replicated
- year_totals: float32 [4, 128], replicated
The draws below stay inside these ranges and needn't reach their ends.
Inputs may be any that keep to these rules, and one draw needn't show every extreme that they name: `day_month`: never falls along the days; month m, for m of 1 to 31, begins at a day from m * 32 - 31 // 2 to m * 32 + 31 // 2, and both ends of that range are taken in every draw. `month_year`: never falls along the months; every year has 1 to 16 months, one exactly that many.
All inputs are finite; a program needn't handle non-finite values.
Results may differ from the reference program's by a relative error of at most 0.0001.
Values sent between devices are 32-bit elements; how exact they have to be, the bound alone decides.
A program may use at most 64 MiB of HBM per device.

```python
import math
import jax
import jax.numpy as jnp
import numpy as np
from jax import lax

DAYS_PER_INDEX = 32
STORE_COUNT = 16
MEASURE_COUNT = 128
CATEGORY_COUNT = 32
REGION_COUNT = 4
TOTAL_DAYS = 1024
PRODUCT_COUNT = 16
TOTAL_MONTHS = 32
YEARS = 4
N_TM = 32


def draw_day_month(key, part):
    half = (DAYS_PER_INDEX - 1) // 2
    inner = TOTAL_MONTHS - 1
    jitter = jax.random.randint(jax.random.fold_in(key, 11), (inner,), -half, half + 1)
    places = jnp.arange(inner, dtype=jnp.int32)
    middle = TOTAL_MONTHS // 2
    jitter = jnp.where(places == 0, -half, jitter)
    jitter = jnp.where(places == middle - 2, -half, jitter)
    jitter = jnp.where(places == middle - 1, half, jitter)
    jitter = jnp.where(places == middle, half, jitter)
    bounds = (places + 1) * DAYS_PER_INDEX + jitter
    days = jnp.arange(TOTAL_DAYS, dtype=jnp.int32)
    return jnp.sum((days[:, None] >= bounds[None, :]).astype(jnp.int32), 1).astype(jnp.int32)


def with_ends(result, rng, low, high):
    dims = result.shape
    place = [jax.random.randint(jax.random.fold_in(rng, axis), (), 0, dims[axis]) for axis in range(len(dims))]
    result = result.at[tuple(place)].set(low)
    longest = dims.index(max(dims))
    place[longest] = (place[longest] + 1) % dims[longest]
    return result.at[tuple(place)].set(high)


def shard_levels(own_key, extent, split, smallest, top_value):
    def one(position, parts):
        draws = jax.random.uniform(jax.random.fold_in(jax.random.fold_in(own_key, 6), position), (parts,), jnp.float32, smallest / len(split), top_value / len(split))
        return jnp.repeat(jnp.exp(draws), extent[position] // parts).reshape((-1,) + (1,) * (len(extent) - position - 1))

    factor_of = one(*split[0])
    for cut in split[1:]:
        factor_of = factor_of * one(*cut)
    return factor_of


def length_profile(number_of, total, bound, slope):
    loads = [(1 << 20) // math.isqrt(grade ** slope) + 1 for grade in range(2, number_of + 1)]
    spare, given = total - bound - (number_of - 1), [1] * (number_of - 1)
    while spare > 0:
        movable = [i for i in range(number_of - 1) if given[i] < bound]
        pool, left = sum([loads[i] for i in movable]), spare
        for i in movable:
            addition = min(bound - given[i], max(1, left * loads[i] // pool), spare)
            given[i] = given[i] + addition
            spare = spare - addition
    return np.array([bound] + given)


def ragged_sizes(rng, amount, total, reach, slope):
    if amount == 2:
        one = jax.random.randint(rng, (), max(1, total - reach), min(reach, total - 1) + 1)
        return jnp.stack([one, total - one])
    sizes = jnp.asarray(length_profile(amount, total, reach, slope), jnp.int32)
    pairs = (amount - 1) // 2
    donor, sink = sizes[1:1 + 2 * pairs:2], sizes[2:2 + 2 * pairs:2]
    margin = jnp.minimum(donor - 1, reach - sink)
    passed = jax.random.randint(jax.random.fold_in(rng, 1), (pairs,), 0, 1 << 20) % (margin + 1)
    sizes = sizes.at[1:1 + 2 * pairs:2].set(donor - passed).at[2:2 + 2 * pairs:2].set(sink + passed)
    return sizes[jax.random.permutation(jax.random.fold_in(rng, 2), amount)]


def bell_draw(own_key, dims, deviation, limit, shards=(), held_as=jnp.bfloat16):
    entries = deviation * jax.random.normal(own_key, dims, jnp.float32)
    if shards:
        entries = entries * shard_levels(own_key, dims, shards, -0.22, 0.18)
    return jnp.clip(entries, -limit, limit).astype(held_as)


def setup_inputs(seed: int = 0) -> dict:
    keys = jax.random.split(jax.random.key(seed), 6)
    sales_records = bell_draw(keys[0], (TOTAL_DAYS, PRODUCT_COUNT, STORE_COUNT, MEASURE_COUNT), 1.0, 6.0, ((0, 32),), jnp.float32)
    day_month = draw_day_month(jax.random.fold_in(keys[5], 71), 0)
    month_year = jnp.searchsorted(jnp.cumsum(ragged_sizes(keys[2], YEARS, TOTAL_MONTHS, 2 * TOTAL_MONTHS // YEARS, 1)), jnp.arange(TOTAL_MONTHS), side="right").astype(jnp.int32)
    product_category = with_ends(jax.random.randint(keys[3], (PRODUCT_COUNT,), 0, CATEGORY_COUNT), jax.random.fold_in(keys[3], 1), 0, CATEGORY_COUNT - 1).astype(jnp.int32)
    store_region = with_ends(jax.random.randint(keys[4], (STORE_COUNT,), 0, REGION_COUNT), jax.random.fold_in(keys[4], 1), 0, REGION_COUNT - 1).astype(jnp.int32)
    return dict(sales_records=sales_records, day_month=day_month, month_year=month_year, product_category=product_category, store_region=store_region)


def onehot(labels, width):
    return (labels[:, None] == jnp.arange(width, dtype=jnp.int32)[None, :]).astype(jnp.float32)

def scaled(sums, counts):
    return sums / jnp.sqrt(counts)

def reference(sales_records, day_month, month_year, product_category, store_region):
    highest = lax.Precision.HIGHEST
    month_hot = onehot(day_month, TOTAL_MONTHS)
    year_hot = onehot(month_year, YEARS)
    category_hot = onehot(product_category, CATEGORY_COUNT)
    region_hot = onehot(store_region, REGION_COUNT)
    daily_blocks = sales_records.reshape(N_TM, DAYS_PER_INDEX, PRODUCT_COUNT, STORE_COUNT, MEASURE_COUNT)
    month_blocks = month_hot.reshape(N_TM, DAYS_PER_INDEX, TOTAL_MONTHS)

    def accumulate(running, pieces):
        day_block, block_hot = pieces
        by_region = jnp.einsum('dpsq,sr->dprq', day_block, region_hot, precision=highest)
        by_category = jnp.einsum('dprq,pc->dcrq', by_region, category_hot, precision=highest)
        return (running + jnp.einsum('dcrq,dm->mcrq', by_category, block_hot, precision=highest), None)
    start_offset = jnp.zeros((TOTAL_MONTHS, CATEGORY_COUNT, REGION_COUNT, MEASURE_COUNT), jnp.float32)
    cube, _ = lax.scan(accumulate, start_offset, (daily_blocks, month_blocks))
    year_cube = jnp.einsum('mcrq,my->ycrq', cube, year_hot, precision=highest)
    month_days = lax.optimization_barrier(jnp.sum(month_hot, 0))
    year_days = jnp.dot(month_days, year_hot, precision=highest)
    category_size = lax.optimization_barrier(jnp.sum(category_hot, 0))
    region_size = lax.optimization_barrier(jnp.sum(region_hot, 0))
    stores = float(STORE_COUNT)
    products = float(PRODUCT_COUNT)

    def four_nodes(detail, period_days):
        cell = period_days[:, None, None] * category_size[None, :, None] * region_size[None, None, :]
        first = scaled(detail, jnp.maximum(cell, 1.0)[..., None])
        by_cat = lax.optimization_barrier(jnp.sum(detail, 2))
        second = scaled(by_cat, jnp.maximum(period_days[:, None] * category_size[None, :] * stores, 1.0)[..., None])
        by_reg = lax.optimization_barrier(jnp.sum(detail, 1))
        third = scaled(by_reg, jnp.maximum(period_days[:, None] * products * region_size[None, :], 1.0)[..., None])
        fourth = scaled(lax.optimization_barrier(jnp.sum(by_reg, 1)), (period_days * products * stores)[:, None])
        return (first, second, third, fourth)
    month_detail, month_category, month_region, month_totals = four_nodes(cube, month_days)
    year_detail, year_category, year_region, year_totals = four_nodes(year_cube, year_days)
    return (month_detail, month_category, month_region, month_totals, year_detail, year_category, year_region, year_totals)
```

```python
import functools

import jax
import jax.numpy as jnp
from jax import lax
from jax.experimental import pallas as pl
from jax.experimental.pallas import tpu as pltpu
from jax.sharding import PartitionSpec as P

MON_DEV = 1
CATEGORY_COUNT = 32
REGION_COUNT = 4


def with_halo(block, sides, width):
    for axis, dim in sides:
        count = lax.axis_size(axis)
        forward = [(i, i + 1) for i in range(count - 1)]
        backward = [(target, source) for source, target in forward]
        low = lax.ppermute(
            lax.slice_in_dim(block, block.shape[dim] - width, None, axis=dim), axis, forward
        )
        high = lax.ppermute(lax.slice_in_dim(block, 0, width, axis=dim), axis, backward)
        block = jnp.concatenate([low, block, high], axis=dim)
    return block


def onehot(labels, width):
    return (labels[:, None] == jnp.arange(width, dtype=jnp.int32)[None, :]).astype(jnp.float32)


def scaled(sums, counts):
    return sums / jnp.sqrt(counts)


def shards(sales_records, day_month, month_year, product_category, store_region):
    highest = lax.Precision.HIGHEST
    day_dev = sales_records.shape[0]
    prod_dev = sales_records.shape[1]
    stores = float(sales_records.shape[2])
    month_width = month_year.shape[0]
    year_width = max(month_width // 8, 2)
    cats_dev = CATEGORY_COUNT // lax.axis_size("prod")
    products = float(prod_dev * lax.axis_size("prod"))
    time_index = lax.axis_index("tm")
    prod_index = lax.axis_index("prod")
    month_hot = onehot(day_month, month_width)
    year_hot = onehot(month_year, year_width)
    category_hot = onehot(product_category, CATEGORY_COUNT)
    region_hot = onehot(store_region, REGION_COUNT)
    local_products = lax.dynamic_slice_in_dim(category_hot, prod_index * prod_dev, prod_dev, 0)
    by_region = jnp.einsum("dpsq,sr->dprq", sales_records, region_hot, precision=highest)
    by_category = jnp.einsum("dprq,pc->dcrq", by_region, local_products, precision=highest)
    month_days = jnp.sum(month_hot, 0)
    year_days = jnp.dot(month_days, year_hot, precision=highest)
    category_size = jnp.sum(category_hot, 0)
    region_size = jnp.sum(region_hot, 0)
    own_days = lax.dynamic_slice_in_dim(month_days, time_index * MON_DEV, MON_DEV, 0)
    own_sizes = lax.dynamic_slice_in_dim(category_size, prod_index * cats_dev, cats_dev, 0)
    local_labels = lax.dynamic_slice_in_dim(day_month, time_index * day_dev, day_dev, 0)
    window_ids = time_index - 1 + jnp.arange(3, dtype=jnp.int32)
    window_hot = (local_labels[:, None] == window_ids[None, :]).astype(jnp.float32)
    partial_value = jnp.einsum("dcrq,dk->kcrq", by_category, window_hot, precision=highest)
    clipped = jnp.clip(window_ids, 0, month_width - 1)
    inside = ((window_ids >= 0) & (window_ids < month_width)).astype(jnp.float32)
    source_years = onehot(month_year[clipped], year_width) * inside[:, None]
    padded = with_halo(partial_value, (("tm", 0),), 1)
    summed = padded[0:1] + padded[2:3] + padded[4:5]
    detail = lax.psum_scatter(summed, "prod", scatter_dimension=1, tiled=True)
    year_part = jnp.einsum("mcrq,my->ycrq", partial_value, source_years, precision=highest)
    year_cube = lax.psum(year_part, ("tm", "prod"))
    cell = own_days[:, None, None] * own_sizes[None, :, None] * region_size[None, None, :]
    month_detail = scaled(detail, jnp.maximum(cell, 1.0)[..., None])
    month_cat = jnp.sum(detail, 2)
    month_category = scaled(
        month_cat, jnp.maximum(own_days[:, None] * own_sizes[None, :] * stores, 1.0)[..., None]
    )
    month_reg = lax.psum(jnp.sum(detail, 1), "prod")
    month_region = scaled(
        month_reg, jnp.maximum(own_days[:, None] * products * region_size[None, :], 1.0)[..., None]
    )
    month_totals = scaled(jnp.sum(month_reg, 1), (own_days * products * stores)[:, None])
    year_cell = year_days[:, None, None] * category_size[None, :, None] * region_size[None, None, :]
    year_detail = scaled(year_cube, jnp.maximum(year_cell, 1.0)[..., None])
    year_cat = jnp.sum(year_cube, 2)
    year_category = scaled(
        year_cat, jnp.maximum(year_days[:, None] * category_size[None, :] * stores, 1.0)[..., None]
    )
    year_reg = jnp.sum(year_cube, 1)
    year_region = scaled(
        year_reg, jnp.maximum(year_days[:, None] * products * region_size[None, :], 1.0)[..., None]
    )
    year_totals = scaled(jnp.sum(year_reg, 1), (year_days * products * stores)[:, None])
    return (
        month_detail,
        month_category,
        month_region,
        month_totals,
        year_detail,
        year_category,
        year_region,
        year_totals,
    )


MESH = pl.DeviceIdType.MESH
TILE = 8
LANES = 128
CHUNK = 4


def three_parts(value):
    high = value.astype(jnp.bfloat16)
    rest = value - high.astype(jnp.float32)
    middle = rest.astype(jnp.bfloat16)
    low = (rest - middle.astype(jnp.float32)).astype(jnp.bfloat16)
    return high, middle, low


def spread(labels_ref, count, index):
    result = jnp.zeros(index.shape, jnp.int32)
    for i in range(count):
        result = jnp.where(index == i, labels_ref[i], result)
    return result


def hot(mask):
    return jnp.where(mask, 1.0, 0.0)


def bits(count):
    return count.bit_length() - 1


def source_ranges(n, months, years):
    longest = 2 * months // years
    result = []
    for y in range(years):
        first = max(y, months - longest * (years - y))
        last = min(longest * (y + 1), months - (years - 1 - y)) - 1
        result.append((max(first - 1, 0), min(last + 1, n - 1)))
    return result


def cube_kernel(
    n, days, products, stores, months, years,
    sales, grid_hbm, year_hbm, category_hbm, region_hbm,
    month_detail, month_category, month_region, month_totals,
    year_detail, year_category, year_region, year_totals,
    day_row, day_grid, month_year, product_category, store_region,
    facts, window, pieces, arrived, totals, from_low, from_high, maps, factors,
    label_sem, fact_sem,
    piece_send, piece_recv, total_send, total_recv, low_send, low_recv, high_send, high_recv,
):
    me = lax.axis_index("tm")
    chunks = products // CHUNK
    rows = products * REGION_COUNT
    group = CHUNK * REGION_COUNT // TILE
    per = years * group
    spacing = n // 2 // per
    owners = [n // 4 + t * spacing + spacing - 1 for t in range(per)]
    ranges = source_ranges(n, months, years)
    within = [(me >= low) & (me <= high) for low, high in ranges]

    def owns(device):
        place = device - n // 4
        return (place >= 0) & (place < n // 2) & (lax.rem(place + n, spacing) == spacing - 1)

    def number(flag):
        return jnp.where(flag, 1, 0)

    owner = owns(me)
    far = (me >= n // 2) & jnp.logical_not(owner)
    mine = jnp.clip((me - n // 4) // spacing, 0, per - 1)

    def fetch(c):
        return pltpu.make_async_copy(sales.at[:, pl.ds(c * CHUNK, CHUNK)], facts.at[c], fact_sem.at[c])

    def remote(source, target, send, recv, device):
        return pltpu.make_async_remote_copy(
            source, target, send, recv, device_id={"tm": device}, device_id_type=MESH
        )

    sources = (grid_hbm.at[me * days // LANES], year_hbm, region_hbm, category_hbm, grid_hbm)
    targets = (day_row, month_year, store_region, product_category, day_grid)
    labels_in = [
        pltpu.make_async_copy(source, target, label_sem.at[i])
        for i, (source, target) in enumerate(zip(sources, targets))
    ]
    for copy in labels_in:
        copy.start()
    for c in range(chunks):
        fetch(c).start()

    barrier = pltpu.get_barrier_semaphore()

    def greet(device):
        pl.semaphore_signal(barrier, 1, device_id={"tm": device}, device_id_type=MESH)

    @pl.when(owner)
    def _():
        @pl.loop(0, n)
        def _(i):
            @pl.when(i != me)
            def _():
                greet(i)

        @pl.loop(0, n)
        def _(i):
            unused = False
            for y, (low, high) in enumerate(ranges):
                unused = unused | ((mine // group == y) & ((i < low) | (i > high)))

            @pl.when(unused)
            def _():
                for c in range(chunks):
                    arrived[c, i] = jnp.zeros((TILE, LANES), jnp.float32)

    @pl.when(jnp.logical_not(owner))
    def _():
        for device in owners:
            greet(device)

        @pl.when((me > 0) & jnp.logical_not(owns(me - 1)))
        def _():
            greet(me - 1)

        @pl.when((me < n - 1) & jnp.logical_not(owns(me + 1)))
        def _():
            greet(me + 1)

    def meet():
        @pl.when(owner)
        def _():
            pl.semaphore_wait(barrier, n - 1)

        @pl.when(jnp.logical_not(owner))
        def _():
            beside = number((me > 0) & jnp.logical_not(owns(me - 1)))
            beside = beside + number((me < n - 1) & jnp.logical_not(owns(me + 1)))
            pl.semaphore_wait(barrier, per + beside)

    def send(c):
        for t, device in enumerate(owners):

            @pl.when(within[t // group] & (me != device))
            def _():
                remote(pieces.at[c * per + t], arrived.at[c, me], piece_send, piece_recv.at[c], device).start()

    for copy in labels_in:
        copy.wait()
    across = CHUNK * stores
    lines = CHUNK * REGION_COUNT
    lane = lax.broadcasted_iota(jnp.int32, (lines, across), 1)
    row = lax.broadcasted_iota(jnp.int32, (lines, across), 0)
    region_of = spread(store_region, stores, lane[:1] & (stores - 1))
    to_region = hot(
        ((row >> bits(REGION_COUNT)) == (lane >> bits(stores))) & ((row & (REGION_COUNT - 1)) == region_of)
    )
    to_region = jnp.concatenate([to_region] * 3, 1).astype(jnp.bfloat16)
    labels = [month_year[jnp.clip(me - 1 + k, 0, months - 1)] for k in range(3)]
    start = lax.rem(me * days, LANES)

    for c in range(chunks):
        fetch(c).wait()
        sums = [jnp.zeros((across, LANES), jnp.float32) for _ in range(3)]
        for d in range(days):
            value = facts[c, d].reshape(across, LANES)
            place = day_row[start + d] - me + 1
            for k in (0, 1) if d < days // 2 else (1, 2):
                sums[k] = sums[k] + value * jnp.where(place == k, 1.0, 0.0)
        held = []
        for k in range(3):
            parts = jnp.concatenate(three_parts(sums[k]), 0)
            held.append(jnp.dot(to_region, parts, preferred_element_type=jnp.float32))
            window[k, c * lines : (c + 1) * lines] = held[k]
        for y in range(years):
            total = jnp.zeros((lines, LANES), jnp.float32)
            for k in range(3):
                total = total + held[k] * jnp.where(labels[k] == y, 1.0, 0.0)
            first = c * per + y * group
            pieces[first : first + group] = total.reshape(group, TILE, LANES)

        @pl.when(far)
        def _():
            if c == 0:
                meet()
            send(c)

    @pl.when(jnp.logical_not(far))
    def _():
        meet()

        @pl.loop(0, chunks)
        def _(c):
            send(c)

    below, above = jnp.maximum(me - 1, 0), jnp.minimum(me + 1, n - 1)
    to_below = remote(window.at[0], from_high, low_send, low_recv, below)
    to_above = remote(window.at[2], from_low, high_send, high_recv, above)

    @pl.when(me > 0)
    def _():
        to_below.start()

    @pl.when(me < n - 1)
    def _():
        to_above.start()

    fill_maps(
        me, products, stores, months, years,
        day_grid, month_year, product_category, store_region, maps, factors,
    )

    def gather(c):
        sent = [high - low + 1 - (low <= owners[t] <= high) for t, (low, high) in
                enumerate(r for r in ranges for _ in range(group))]
        for count in sorted(set(sent)):
            is_count = False
            for t in range(per):
                if sent[t] == count:
                    is_count = is_count | (mine == t)

            @pl.when(is_count)
            def _():
                everything = arrived.at[c, pl.ds(0, count)]
                pltpu.make_async_copy(everything, everything, piece_recv.at[c]).wait()

        inside = False
        for t in range(per):
            if ranges[t // group][0] <= owners[t] <= ranges[t // group][1]:
                inside = inside | (mine == t)

        @pl.when(inside)
        def _():
            arrived[c, me] = pieces[c * per + mine]

        sums = [arrived[c, j] for j in range(n)]
        while len(sums) > 1:
            sums = [a + b for a, b in zip(sums[::2], sums[1::2])]
        slot = (mine // group) * (rows // TILE) + c * group + lax.rem(mine, group)
        totals[slot] = sums[0]

        @pl.loop(0, n)
        def _(i):
            @pl.when(i != me)
            def _():
                remote(totals.at[slot], totals.at[slot], total_send, total_recv, i).start()

    @pl.when(owner)
    def _():
        for c in range(chunks - 1):
            gather(c)

    @pl.when(me > 0)
    def _():
        to_below.wait_send()
        to_above.wait_recv()
        window[1] += from_low[...]

    @pl.when(me < n - 1)
    def _():
        to_above.wait_send()
        to_below.wait_recv()
        window[1] += from_high[...]

    def place(value, period, refs):
        parts = jnp.concatenate(three_parts(value), 0)
        mapped = jnp.dot(maps[...], parts, preferred_element_type=jnp.float32) * factors[period]
        first = 0
        for ref, count in zip(refs, (CATEGORY_COUNT * REGION_COUNT, CATEGORY_COUNT, REGION_COUNT, 1)):
            begin = max(period - 1, 0) * count
            ref[begin : begin + count] = mapped[first : first + count]
            first += count

    place(window[1], 0, (month_detail, month_category, month_region, month_totals))

    @pl.when(owner)
    def _():
        gather(chunks - 1)

    sends = sum(number(flag) for flag in within) * group
    sends = sends - sum(number(within[t // group] & (me == device)) for t, device in enumerate(owners))
    for count in range(per + 1):

        @pl.when(sends == count)
        def _():
            if count:
                sent = pieces.at[pl.ds(0, count * chunks)]
                pltpu.make_async_copy(sent, sent, piece_send).wait()

    @pl.when(owner)
    def _():
        others = totals.at[pl.ds(0, (per - 1) * chunks)]
        pltpu.make_async_copy(others, others, total_recv).wait()

    @pl.when(jnp.logical_not(owner))
    def _():
        pltpu.make_async_copy(totals, totals, total_recv).wait()

    for y in range(years):
        value = totals[pl.ds(y * (rows // TILE), rows // TILE)].reshape(rows, LANES)
        place(value, y + 1, (year_detail, year_category, year_region, year_totals))

    @pl.when(owner)
    def _():
        for c in range(chunks):
            others = pieces.at[pl.ds(0, n - 1)]
            pltpu.make_async_copy(others, others, total_send).wait()


def fill_maps(
    me, products, stores, months, years,
    day_grid, month_year, product_category, store_region, maps, factors,
):
    rows = products * REGION_COUNT
    shift, low = bits(REGION_COUNT), REGION_COUNT - 1
    lane = lax.broadcasted_iota(jnp.int32, (1, rows), 1)
    lane_category = spread(product_category, products, lane >> shift)
    lane_region = lane & low

    def row(count):
        return lax.broadcasted_iota(jnp.int32, (count, rows), 0)

    cells = CATEGORY_COUNT * REGION_COUNT
    to_cell = hot(((row(cells) >> shift) == lane_category) & ((row(cells) & low) == lane_region))
    to_cat = hot(row(CATEGORY_COUNT) == lane_category)
    to_reg = hot((row(TILE) == lane_region) | (row(TILE) == REGION_COUNT))
    cell_cat = jnp.sum(to_cell, 1, keepdims=True)
    cat_size = jnp.sum(to_cat, 1, keepdims=True) * (1.0 / REGION_COUNT)
    region_size = []
    for r in range(REGION_COUNT):
        size = jnp.int32(0)
        for s in range(stores):
            size = size + jnp.where(store_region[s] == r, 1, 0)
        region_size.append(size.astype(jnp.float32))

    def sizes(count):
        place = lax.broadcasted_iota(jnp.int32, (count, 1), 0) & low
        result = jnp.zeros((count, 1), jnp.float32)
        for r in range(REGION_COUNT):
            result = jnp.where(place == r, region_size[r], result)
        return result

    cell_reg, reg_size = sizes(cells), sizes(TILE)
    joined = jnp.concatenate([to_cell, to_cat, to_reg], 0)
    maps[...] = jnp.concatenate([joined] * 3, 1).astype(jnp.bfloat16)
    days = day_grid[...]
    years_of = jnp.zeros(days.shape, jnp.int32)
    for m in range(months):
        years_of = jnp.where(days == m, month_year[m], years_of)
    last = lax.broadcasted_iota(jnp.int32, (TILE, 1), 0)
    for i, mask in enumerate([days == me] + [years_of == y for y in range(years)]):
        period = jnp.sum(jnp.sum(hot(mask), 1, keepdims=True), 0, keepdims=True)
        tail = jnp.where(
            last == REGION_COUNT,
            period * float(products * stores),
            jnp.maximum(period * float(products) * reg_size, 1.0),
        )
        counts = jnp.concatenate(
            [
                jnp.maximum(period * cell_cat * cell_reg, 1.0),
                jnp.maximum(period * cat_size * float(stores), 1.0),
                tail,
            ],
            0,
        )
        factors[i] = jnp.broadcast_to(1.0 / jnp.sqrt(counts), (counts.shape[0], LANES))


def finish_kernel(*refs):
    count = len(refs) // 2
    copies = [pltpu.make_async_copy(refs[i], refs[count + i], refs[-1].at[i]) for i in range(count)]
    for copy in copies:
        copy.start()
    for copy in copies:
        copy.wait()


def kernels(sales_records, day_month, month_year, product_category, store_region):
    n = lax.axis_size("tm")
    days, products, stores, _ = sales_records.shape
    months = month_year.shape[0]
    years = max(months // 8, 2)
    rows = products * REGION_COUNT
    f32 = jnp.float32
    hbm = pl.BlockSpec(memory_space=pl.ANY)
    vmem = pl.BlockSpec(memory_space=pltpu.VMEM)
    dma = pltpu.SemaphoreType.DMA
    i32 = jnp.int32
    cells = CATEGORY_COUNT * REGION_COUNT
    lines = cells + CATEGORY_COUNT + TILE
    shapes = [(cells, LANES), (CATEGORY_COUNT, LANES), (REGION_COUNT, LANES), (1, LANES)]
    shapes += [(years * count, LANES) for count, _ in shapes]
    grid = day_month.reshape(-1, LANES)
    results = pl.pallas_call(
        functools.partial(cube_kernel, n, days, products, stores, months, years),
        out_shape=tuple(pltpu.VMEM(s, f32) for s in shapes),
        in_specs=[hbm] * 5,
        out_specs=(vmem,) * 8,
        scratch_shapes=[
            pltpu.SMEM((LANES,), i32),
            pltpu.VMEM(grid.shape, i32),
            pltpu.SMEM(month_year.shape, i32),
            pltpu.SMEM(product_category.shape, i32),
            pltpu.SMEM(store_region.shape, i32),
            pltpu.VMEM((products // CHUNK, days, CHUNK, stores, LANES), f32),
            pltpu.VMEM((3, rows, LANES), f32),
            pltpu.VMEM((n, TILE, LANES), f32),
            pltpu.VMEM((products // CHUNK, n, TILE, LANES), f32),
            pltpu.VMEM((n, TILE, LANES), f32),
            pltpu.VMEM((rows, LANES), f32),
            pltpu.VMEM((rows, LANES), f32),
            pltpu.VMEM((lines, 3 * rows), jnp.bfloat16),
            pltpu.VMEM((years + 1, lines, LANES), f32),
            dma((5,)),
            dma((products // CHUNK,)),
        ]
        + [dma, dma((products // CHUNK,))]
        + [dma] * 6,
        compiler_params=pltpu.CompilerParams(collective_id=0, has_side_effects=True),
        name="cube",
    )(sales_records, grid, month_year, product_category, store_region)
    outs = pl.pallas_call(
        finish_kernel,
        out_shape=tuple(jax.ShapeDtypeStruct(s, f32) for s in shapes),
        in_specs=[vmem] * 8,
        out_specs=(hbm,) * 8,
        scratch_shapes=[dma((8,))],
        compiler_params=pltpu.CompilerParams(vmem_limit_bytes=2**20),
        name="finish",
    )(*results)
    tails = [(CATEGORY_COUNT, REGION_COUNT, LANES), (CATEGORY_COUNT, LANES), (REGION_COUNT, LANES), (LANES,)]
    return tuple(
        out.reshape((1 if i < 4 else years,) + tails[i % 4]) for i, out in enumerate(outs)
    )


def power(count):
    return count & (count - 1) == 0


def body(*args):
    days, products, stores, lanes = args[0].shape
    n = lax.axis_size("tm")
    tiles = max(args[2].shape[0] // 8, 2) * products * REGION_COUNT // TILE
    fits = (
        lax.axis_size("prod") == 1
        and tiles == n
        and args[2].shape[0] == n
        and power(n)
        and power(stores)
        and stores % TILE == 0
        and products % CHUNK == 0
        and lanes == LANES
        and args[1].shape[0] % (TILE * LANES) == 0
        and LANES % days == 0
        and n // 2 % (tiles * CHUNK // products) == 0
    )
    return kernels(*args) if fits else shards(*args)


def solution(mesh):
    placed = (P("tm", "prod", None, None), P(), P(), P(), P())
    return jax.shard_map(
        body,
        mesh=mesh,
        in_specs=placed,
        out_specs=(
            P("tm", "prod", None, None),
            P("tm", "prod", None),
            P("tm", None, None),
            P("tm", None),
            P(),
            P(),
            P(),
            P(),
        ),
        check_vma=False,
    )
```
